8 devices in a mesh: rep: 1 (over z), pp: 8 (over x, y, core).
Axes of the slice: x: 2, y: 2, z: 1, core: 2. Of those that a mesh axis runs over, the one named last changes fastest.
Arguments:
- x: bfloat16 [16, 512, 512], P('rep')
- dy: bfloat16 [16, 512, 512], P('rep')
- w_gate: bfloat16 [8, 512, 1280], P('pp')
- w_up: bfloat16 [8, 512, 1280], P('pp')
- w_down: bfloat16 [8, 1280, 512], P('pp')
Outputs:
- output 1: bfloat16 [8, 512, 1280], P(('rep', 'pp'))
- output 2: bfloat16 [8, 512, 1280], P(('rep', 'pp'))
- output 3: bfloat16 [8, 1280, 512], P(('rep', 'pp'))
All inputs are finite; a program needn't handle non-finite values.
Results may differ from the reference program's by a relative error of at most 0.0266.
Values are sent between devices in bfloat16 or wider.
A program may use at most 2 GiB of HBM per device.

```python
import jax
import jax.numpy as jnp
from jax import lax

MICRO = 16
TOKENS = 512
D = 512
FF = 1280
LAYERS = 8
NAMES = ("w_gate", "w_up", "w_down")
SHAPES = {"w_gate": (LAYERS, D, FF), "w_up": (LAYERS, D, FF), "w_down": (LAYERS, FF, D)}


def bump(key, n, height):
    away = (jnp.arange(n, dtype=jnp.int32) - jax.random.randint(key, (), 0, n, jnp.int32)) % n
    return jnp.where(away < n // 8, height, 1.0)


def together(key, own, strength):
    shared = jax.random.normal(key, own.shape[1:], jnp.float32)
    return (own + strength * shared) * lax.rsqrt(1 + strength * strength)


def setup_inputs(seed: int = 0, part: int = 0) -> dict:
    kx, kdy, ka, kb, kz, kf, kh, kl, *kw = jax.random.split(jax.random.key(seed), 8 + len(NAMES))
    kx, kdy, ka, kb = (jax.random.fold_in(k, part) for k in (kx, kdy, ka, kb))
    shape = (MICRO, TOKENS, D)
    much_x, much_dy = jax.random.uniform(kz, (2,), jnp.float32, 0.0, 1.0)
    layers = 2.0 ** jax.random.uniform(kl, (LAYERS, 1, 1), jnp.float32, -1.0, 1.0)
    x = together(ka, jax.random.normal(kx, shape, jnp.float32), much_x) * bump(kf, D, 4.0)
    dy = together(kb, jax.random.normal(kdy, shape, jnp.float32), much_dy)
    drawn = {"x": x.astype(jnp.bfloat16), "dy": (dy * (MICRO * TOKENS) ** -0.5).astype(jnp.bfloat16)}
    for key, name in zip(kw, NAMES, strict=True):
        w = jax.random.normal(key, SHAPES[name], jnp.float32) * SHAPES[name][1] ** -0.5
        drawn[name] = (w * {"w_gate": 1.0, "w_up": bump(kh, FF, 4.0), "w_down": layers}[name]).astype(jnp.bfloat16)
    return drawn


def matmul(a, w):
    return jnp.dot(a, w, preferred_element_type=jnp.float32).astype(jnp.bfloat16)


def normed(h):
    wide = h.astype(jnp.float32)
    scale = lax.rsqrt(jnp.mean(wide**2, -1, keepdims=True) + 1e-6)
    return (wide * scale).astype(jnp.bfloat16)


def layer(h, w):
    a = normed(h)
    gate = jnp.dot(a, w["w_gate"], preferred_element_type=jnp.float32)
    up = jnp.dot(a, w["w_up"], preferred_element_type=jnp.float32)
    return h + matmul((jax.nn.silu(gate) * up).astype(jnp.bfloat16), w["w_down"])


def stack(weights, h):
    return lax.scan(lambda h, w: (layer(h, w), None), h, weights)[0]


def reference(x, dy, w_gate, w_up, w_down):
    weights = dict(zip(NAMES, (w_gate, w_up, w_down), strict=True))

    def take(so_far, one):
        h, by_y = one
        _, back = jax.vjp(lambda w: stack(w, h), weights)
        return jax.tree.map(lambda total, term: total + term.astype(jnp.float32), so_far, back(by_y)[0]), None

    none_yet = {name: jnp.zeros(w.shape, jnp.float32) for name, w in weights.items()}
    by_weights, _ = lax.scan(take, none_yet, (x, dy))
    return tuple(by_weights[name].astype(jnp.bfloat16) for name in NAMES)
```

```python
import functools

import jax
import jax.numpy as jnp
from jax import lax
from jax.experimental import pallas as pl
from jax.experimental.pallas import tpu as pltpu
from jax.sharding import PartitionSpec as P

f32, bf16 = jnp.float32, jnp.bfloat16
MESH = pl.DeviceIdType.MESH
ROWS = 256
BLOCK = 256
RING = 8
LEAD = (16, 14, 11, 10, 7, 5, 2, 0)
VMEM_BYTES = 64 * 2**20 - 2**16


def mm(a, b):
    return jnp.dot(a, b, preferred_element_type=f32)


def mm_nt(a, b):
    return lax.dot_general(a, b, (((1,), (1,)), ((), ())), preferred_element_type=f32)


def mm_tn(a, b):
    return lax.dot_general(a, b, (((0,), (0,)), ((), ())), preferred_element_type=f32)


def norm_of(h):
    wide = h.astype(f32)
    return wide, lax.rsqrt(jnp.mean(wide * wide, -1, keepdims=True) + 1e-6)


def blocks(ff):
    return [slice(at, at + BLOCK) for at in range(0, ff, BLOCK)]


def forward(h, wg, wu, wd, hidden):
    wide, scale = norm_of(h)
    a = (wide * scale).astype(bf16)
    for c in blocks(hidden.shape[1]):
        gate, up = mm(a, wg[:, c]), mm(a, wu[:, c])
        hidden[:, c] = (gate * jax.nn.sigmoid(gate) * up).astype(bf16)
    return h + mm(hidden[...], wd[...]).astype(bf16)


def backward(h, by_y, wg, wu, wd, a_all, hid_all, by_gate, by_up, rows):
    wide, scale = norm_of(h)
    a = (wide * scale).astype(bf16)
    a_all[rows, :] = a
    for c in blocks(hid_all.shape[1]):
        gate, up = mm(a, wg[:, c]), mm(a, wu[:, c])
        by_hid = mm_nt(by_y, wd[c, :]).astype(bf16).astype(f32)
        sig = jax.nn.sigmoid(gate)
        silu = gate * sig
        hid_all[rows, c] = (silu * up).astype(bf16)
        by_up[rows, c] = (by_hid * silu).astype(bf16)
        by_gate[rows, c] = ((by_hid * up) * (sig + silu * (1.0 - sig))).astype(bf16)
    return wide, scale


def backward_input(wide, scale, by_y, wg, wu, by_gate, by_up, rows):
    by_a = mm_nt(by_gate[rows, :], wg[...]).astype(bf16) + mm_nt(by_up[rows, :], wu[...]).astype(bf16)
    by_a = by_a.astype(f32)
    inner = jnp.sum(by_a * wide, -1, keepdims=True) * (1.0 / wide.shape[1])
    return by_y + (by_a * scale - wide * (scale * scale * scale * inner)).astype(bf16)


def kernel(stages, chunks, per, x, dy, wg, wu, wd, o_gate, o_up, o_down, kept, came, f_out, b_out, hidden, a_all, hid_all, by_gate, by_up,
           acc, f_in, b_in, f_sent, b_sent):
    me = lax.axis_index("pp")
    first, last = me == 0, me == stages - 1
    lead = sum(jnp.where(me == i, n, 0) for i, n in enumerate(LEAD))
    ff = hidden.shape[1]

    barrier = pltpu.get_barrier_semaphore()

    @pl.when(jnp.logical_not(last))
    def _():
        pl.semaphore_signal(barrier, inc=1, device_id={"pp": me + 1}, device_id_type=MESH)

    @pl.when(jnp.logical_not(first))
    def _():
        pl.semaphore_signal(barrier, inc=1, device_id={"pp": me - 1}, device_id_type=MESH)

    pl.semaphore_wait(barrier, jnp.where(first | last, 1, 2))

    def load(source, target, sems):
        def one(k, _):
            pltpu.make_async_copy(source.at[k], target.at[k], sems.at[k]).start()
            return 0

        lax.fori_loop(0, chunks, one, 0)

    @pl.when(first)
    def _():
        load(x, kept, f_in)

    @pl.when(last)
    def _():
        load(dy, came, b_in)

    acc[...] = jnp.zeros_like(acc)

    def send(k, out, into, sent, arrived, to):
        slot = lax.rem(k, RING)
        return pltpu.make_async_remote_copy(
            src_ref=out.at[slot], dst_ref=into.at[k], send_sem=sent.at[slot], recv_sem=arrived.at[k], device_id={"pp": to}, device_id_type=MESH
        )

    def f_send(k):
        return send(k, f_out, kept, f_sent, f_in, me + 1)

    def b_send(k):
        return send(k, b_out, came, b_sent, b_in, me - 1)

    def arrived(k, into, sems):
        pltpu.make_async_copy(into.at[k], into.at[k], sems.at[k]).wait()

    def take(t, _):
        k = t

        @pl.when(k < chunks)
        def _():
            arrived(k, kept, f_in)

        @pl.when((k < chunks) & jnp.logical_not(last))
        def _():
            @pl.when(k >= RING)
            def _():
                f_send(k - RING).wait_send()

            f_out[lax.rem(k, RING)] = forward(kept[k], wg, wu, wd, hidden)
            f_send(k).start()

        j = t - lead

        @pl.when((j >= 0) & (j < chunks))
        def _():
            arrived(j, came, b_in)
            rows = pl.ds(pl.multiple_of(lax.rem(j, per) * ROWS, ROWS), ROWS)
            by_y = came[j]
            wide, scale = backward(kept[j], by_y, wg, wu, wd, a_all, hid_all, by_gate, by_up, rows)

            @pl.when(jnp.logical_not(first))
            def _():
                @pl.when(j >= RING)
                def _():
                    b_send(j - RING).wait_send()

                b_out[lax.rem(j, RING)] = backward_input(*norm_of(kept[j]), came[j], wg, wu, by_gate, by_up, rows)
                b_send(j).start()

            @pl.when(lax.rem(j, per) == per - 1)
            def _():
                for c in blocks(ff):
                    by_out = jnp.concatenate([came[j - per + 1 + i] for i in range(per)], axis=0)
                    acc[0, :, c] += mm_tn(a_all[...], by_gate[:, c]).astype(bf16).astype(f32)
                    acc[1, :, c] += mm_tn(a_all[...], by_up[:, c]).astype(bf16).astype(f32)
                    acc[2, :, c] += mm_tn(by_out, hid_all[:, c]).astype(bf16).astype(f32)

        return 0

    lax.fori_loop(0, chunks + lead, take, 0)

    def drain(i, _):
        @pl.when(jnp.logical_not(last))
        def _():
            f_send(chunks - RING + i).wait_send()

        @pl.when(jnp.logical_not(first))
        def _():
            b_send(chunks - RING + i).wait_send()

        return 0

    lax.fori_loop(0, RING, drain, 0)
    o_gate[...] = acc[0].astype(bf16)
    o_up[...] = acc[1].astype(bf16)
    o_down[...] = acc[2].astype(bf16)


def solution(mesh):
    stages = mesh.shape["pp"]

    def step(x, dy, w_gate, w_up, w_down):
        micro, tokens, d = x.shape
        ff = w_gate.shape[2]
        per = tokens // ROWS
        chunks = micro * per
        x, dy = (v.reshape(chunks, ROWS, d) for v in (x, dy))
        vmem, anywhere = pl.BlockSpec(memory_space=pltpu.VMEM), pl.BlockSpec(memory_space=pl.ANY)
        by_gate, by_up, by_down = pl.pallas_call(
            functools.partial(kernel, stages, chunks, per),
            out_shape=[jax.ShapeDtypeStruct((d, ff), bf16)] * 3,
            in_specs=[anywhere] * 2 + [vmem] * 3,
            out_specs=[vmem] * 3,
            scratch_shapes=[
                pltpu.VMEM((chunks, ROWS, d), bf16),
                pltpu.VMEM((chunks, ROWS, d), bf16),
                pltpu.VMEM((RING, ROWS, d), bf16),
                pltpu.VMEM((RING, ROWS, d), bf16),
                pltpu.VMEM((ROWS, ff), bf16),
                pltpu.VMEM((tokens, d), bf16),
                pltpu.VMEM((tokens, ff), bf16),
                pltpu.VMEM((tokens, ff), bf16),
                pltpu.VMEM((tokens, ff), bf16),
                pltpu.VMEM((3, d, ff), f32),
                pltpu.SemaphoreType.DMA((chunks,)),
                pltpu.SemaphoreType.DMA((chunks,)),
                pltpu.SemaphoreType.DMA((RING,)),
                pltpu.SemaphoreType.DMA((RING,)),
            ],
            compiler_params=pltpu.CompilerParams(collective_id=0, has_side_effects=True, vmem_limit_bytes=VMEM_BYTES),
            cost_estimate=pl.CostEstimate(flops=22 * micro * tokens * d * ff, bytes_accessed=16 * d * ff, transcendentals=0),
        )(x, dy, w_gate[0], w_up[0], w_down[0])
        return by_gate[None], by_up[None], by_down.T[None]

    return jax.shard_map(
        step,
        mesh=mesh,
        in_specs=(P("rep", None, None),) * 2 + (P("pp", None, None),) * 3,
        out_specs=(P(("rep", "pp"), None, None),) * 3,
        check_vma=False,
    )
```

```python
import functools

import jax
import jax.numpy as jnp
from jax import lax
from jax.experimental import pallas as pl
from jax.experimental.pallas import tpu as pltpu
from jax.sharding import PartitionSpec as P

f32, bf16 = jnp.float32, jnp.bfloat16
MESH = pl.DeviceIdType.MESH
ROWS = 256
BLOCK = 256
RING = 4
LEAD = (28, 24, 15, 13, 8, 6, 2, 0)
CROSS = 3
F_RELAY, B_RELAY = 0, 7
F_FAR, B_FAR = 144, 112
F_SPLIT, B_SPLIT = (7, 31), (0, 20)
F_BEHIND, B_BEHIND = 10, 6
MERGED = ()
STASHED, SLOTS = (4, 5, 6), 9
VMEM_BYTES = 60 * 2**20


def mm(a, b):
    return jnp.dot(a, b, preferred_element_type=f32)


def mm_nt(a, b):
    return lax.dot_general(a, b, (((1,), (1,)), ((), ())), preferred_element_type=f32)


def mm_tn(a, b):
    return lax.dot_general(a, b, (((0,), (0,)), ((), ())), preferred_element_type=f32)


def norm_of(h):
    wide = h.astype(f32)
    return wide, lax.rsqrt(jnp.mean(wide * wide, -1, keepdims=True) + 1e-6)


def blocks(ff):
    return [slice(at, at + BLOCK) for at in range(0, ff, BLOCK)]


def forward(h, wg, wu, wd, hidden, stash=None):
    wide, scale = norm_of(h)
    a = (wide * scale).astype(bf16)
    for c in blocks(hidden.shape[1]):
        gate, up = mm(a, wg[:, c]), mm(a, wu[:, c])
        if stash is not None:
            stash[0, :, c], stash[1, :, c] = gate, up
        hidden[:, c] = (gate * jax.nn.sigmoid(gate) * up).astype(bf16)
    return h + mm(hidden[...], wd[...]).astype(bf16)


def backward(h, by_y, wg, wu, wd, a_all, hid_all, by_gate, by_up, rows, stash=None):
    wide, scale = norm_of(h)
    a = (wide * scale).astype(bf16)
    a_all[rows, :] = a
    for c in blocks(hid_all.shape[1]):
        gate, up = (mm(a, wg[:, c]), mm(a, wu[:, c])) if stash is None else (stash[0, :, c], stash[1, :, c])
        by_hid = mm_nt(by_y, wd[c, :]).astype(bf16).astype(f32)
        sig = jax.nn.sigmoid(gate)
        silu = gate * sig
        hid_all[rows, c] = (silu * up).astype(bf16)
        by_up[rows, c] = (by_hid * silu).astype(bf16)
        by_gate[rows, c] = ((by_hid * up) * (sig + silu * (1.0 - sig))).astype(bf16)
    return wide, scale


def backward_input(wide, scale, by_y, wg, wu, by_gate, by_up, rows):
    by_a = mm_nt(by_gate[rows, :], wg[...]).astype(bf16) + mm_nt(by_up[rows, :], wu[...]).astype(bf16)
    by_a = by_a.astype(f32)
    inner = jnp.sum(by_a * wide, -1, keepdims=True) * (1.0 / wide.shape[1])
    return by_y + (by_a * scale - wide * (scale * scale * scale * inner)).astype(bf16)


def kernel(stages, chunks, per, x, dy, wg, wu, wd, o_gate, o_up, o_down, kept, came, f_out, b_out, hidden, a_all, hid_all,
           acc, acc_down, relay, stash, f_in, b_in, f_sent, b_sent, f_round, b_round, r_in, r_sent, x_sent):
    me = lax.axis_index("pp")
    first, last = me == 0, me == stages - 1
    lead = sum(jnp.where(me == i, n, 0) for i, n in enumerate(LEAD))
    ff = hidden.shape[1]
    by_gate, by_up = o_gate, o_up

    barrier = pltpu.get_barrier_semaphore()

    @pl.when(jnp.logical_not(last))
    def _():
        pl.semaphore_signal(barrier, inc=1, device_id={"pp": me + 1}, device_id_type=MESH)

    @pl.when(jnp.logical_not(first))
    def _():
        pl.semaphore_signal(barrier, inc=1, device_id={"pp": me - 1}, device_id_type=MESH)

    pairs = [(CROSS, F_RELAY), (F_RELAY, CROSS + 1), (CROSS + 1, B_RELAY), (B_RELAY, CROSS)]
    for one, other in pairs + [(b, a) for a, b in pairs]:

        @pl.when(me == one)
        def _():
            pl.semaphore_signal(barrier, inc=1, device_id={"pp": other}, device_id_type=MESH)

    greeted = jnp.where(first | last, 1, 2) + sum(jnp.where(me == one, 1, 0) for pair in pairs for one in pair)
    pl.semaphore_wait(barrier, greeted)

    def load(source, target, sems):
        def one(k, _):
            pltpu.make_async_copy(source.at[k], target.at[k], sems.at[k]).start()
            return 0

        lax.fori_loop(0, chunks, one, 0)

    @pl.when(first)
    def _():
        load(x, kept, f_in)

    @pl.when(last)
    def _():
        load(dy, came, b_in)

    acc[...] = jnp.zeros_like(acc)
    acc_down[...] = jnp.zeros_like(acc_down)

    def send(k, out, into, sent, arrived, to):
        slot = lax.rem(k, RING)
        return pltpu.make_async_remote_copy(
            src_ref=out.at[slot], dst_ref=into.at[k], send_sem=sent.at[slot], recv_sem=arrived.at[k], device_id={"pp": to}, device_id_type=MESH
        )

    def f_split(k):
        return (k >= F_SPLIT[0]) & (k < F_SPLIT[1])

    def b_split(k):
        return (k >= B_SPLIT[0]) & (k < B_SPLIT[1])

    f_cut, b_cut = ((pl.ds(0, ROWS - far), pl.ds(ROWS - far, far), pl.ds(0, far), span[0]) for far, span in ((F_FAR, F_SPLIT), (B_FAR, B_SPLIT)))

    def halves(k, out, into, sent, arrived, to, by, cut):
        slot = lax.rem(k, RING)
        near, far, at, base = cut
        return (
            pltpu.make_async_remote_copy(
                src_ref=out.at[slot, near], dst_ref=into.at[k, near], send_sem=sent.at[slot], recv_sem=arrived.at[k], device_id={"pp": to},
                device_id_type=MESH,
            ),
            pltpu.make_async_remote_copy(
                src_ref=out.at[slot, far], dst_ref=relay.at[k - base, at], send_sem=x_sent.at[slot], recv_sem=r_in.at[k], device_id={"pp": by},
                device_id_type=MESH,
            ),
        )

    def pass_on(k, into, round_, to, cut):
        return pltpu.make_async_remote_copy(
            src_ref=relay.at[k - cut[3], cut[2]], dst_ref=into.at[k, cut[1]], send_sem=r_sent.at[k], recv_sem=round_.at[k], device_id={"pp": to},
            device_id_type=MESH,
        )

    f_pass = lambda k: pass_on(k, kept, f_round, CROSS + 1, f_cut)
    b_pass = lambda k: pass_on(k, came, b_round, CROSS, b_cut)

    def either(split, whole, parts):
        @pl.when(jnp.logical_not(split))
        def _():
            whole()

        @pl.when(split)
        def _():
            parts()

    def f_do(k, what):
        def parts():
            for copy in halves(k, f_out, kept, f_sent, f_in, CROSS + 1, F_RELAY, f_cut):
                what(copy)

        either((me == CROSS) & f_split(k), lambda: what(send(k, f_out, kept, f_sent, f_in, me + 1)), parts)

    def b_do(k, what):
        def parts():
            for copy in halves(k, b_out, came, b_sent, b_in, CROSS, B_RELAY, b_cut):
                what(copy)

        either((me == CROSS + 1) & b_split(k), lambda: what(send(k, b_out, came, b_sent, b_in, me - 1)), parts)

    start, wait_send = lambda copy: copy.start(), lambda copy: copy.wait_send()

    def arrived(k, into, sems, round_, split, cut):
        def parts():
            for rows, sem in zip(cut, (sems, round_)):
                pltpu.make_async_copy(into.at[k, rows], into.at[k, rows], sem.at[k]).wait()

        either(split, lambda: pltpu.make_async_copy(into.at[k], into.at[k], sems.at[k]).wait(), parts)

    stashes = sum(jnp.where(me == i, 1, 0) for i in STASHED) > 0

    merges = sum([jnp.where(me == i, 1, 0) for i in MERGED], 0) > 0
    middle = jnp.logical_not(first | stashes)

    def take(t, _):
        for by, behind, split, copy, cut in ((F_RELAY, F_BEHIND, f_split, f_pass, f_cut), (B_RELAY, B_BEHIND, b_split, b_pass, b_cut)):

            @pl.when((me == by) & (t >= behind) & split(t - behind))
            def _():
                here = relay.at[t - behind - cut[3], cut[2]]
                pltpu.make_async_copy(here, here, r_in.at[t - behind]).wait()
                copy(t - behind).start()

        k, j = t, t - lead
        has_f, has_b = (k < chunks) & jnp.logical_not(last), (j >= 0) & (j < chunks)
        rows = pl.ds(pl.multiple_of(lax.rem(j + chunks, per) * ROWS, ROWS), ROWS)
        out = jnp.logical_not(first)

        @pl.when(k < chunks)
        def _():
            arrived(k, kept, f_in, f_round, (me == CROSS + 1) & f_split(k), f_cut)

        @pl.when(has_f & (k >= RING))
        def _():
            f_do(k - RING, wait_send)

        def await_b():
            arrived(j, came, b_in, b_round, (me == CROSS) & b_split(j), b_cut)

            @pl.when(out & (j >= RING))
            def _():
                b_do(j - RING, wait_send)

        def work(forth, back, whole=True, stashed=False):
            if back:
                kept_of = stash.at[lax.rem(j, SLOTS)] if stashed else None
                wide, scale = backward(kept[j], came[j], wg, wu, wd, a_all, hid_all, by_gate, by_up, rows, kept_of)
                if whole:
                    b_out[lax.rem(j, RING)] = backward_input(wide, scale, came[j], wg, wu, by_gate, by_up, rows)
            if forth:
                f_out[lax.rem(k, RING)] = forward(kept[k], wg, wu, wd, hidden, stash.at[lax.rem(k, SLOTS)] if stashed else None)

        joint = has_f & has_b & merges
        if set(MERGED):
            pl.when(joint)(await_b)
            if 0 in MERGED:
                pl.when(joint & first)(lambda: work(True, True, whole=False))
            if set(MERGED) - set(STASHED) - {0}:
                pl.when(joint & middle)(lambda: work(True, True))
            if set(MERGED) & set(STASHED):
                pl.when(joint & stashes)(lambda: work(True, True, stashed=True))

        pl.when(has_f & jnp.logical_not(joint))(lambda: work(True, False, stashed=True))

        @pl.when(has_f)
        def _():
            f_do(k, start)

        only_b = has_b & jnp.logical_not(joint)
        pl.when(only_b)(await_b)
        pl.when(only_b & first)(lambda: work(False, True, whole=False))
        pl.when(only_b & middle)(lambda: work(False, True))
        pl.when(only_b & stashes)(lambda: work(False, True, stashed=True))

        @pl.when(has_b & out)
        def _():
            b_do(j, start)

        @pl.when(has_b & (lax.rem(j + chunks, per) == per - 1))
        def _():
            by_out = jnp.concatenate([came[j - per + 1 + i] for i in range(per)], axis=0)
            for c in blocks(ff):
                acc[0, :, c] += mm_tn(a_all[...], by_gate[:, c]).astype(bf16).astype(f32)
                acc[1, :, c] += mm_tn(a_all[...], by_up[:, c]).astype(bf16).astype(f32)
                acc_down[c, :] += mm_tn(hid_all[:, c], by_out).astype(bf16).astype(f32)

        return 0

    steps = chunks + jnp.maximum(lead, jnp.where(me == F_RELAY, F_BEHIND, jnp.where(me == B_RELAY, B_BEHIND, 0)))
    lax.fori_loop(0, steps, take, 0)

    def drain(i, _):
        @pl.when(jnp.logical_not(last))
        def _():
            f_do(chunks - RING + i, wait_send)

        @pl.when(jnp.logical_not(first))
        def _():
            b_do(chunks - RING + i, wait_send)

        return 0

    lax.fori_loop(0, RING, drain, 0)
    for by, span, copy in ((F_RELAY, F_SPLIT, f_pass), (B_RELAY, B_SPLIT, b_pass)):

        @pl.when(me == by)
        def _():
            def passed(k, _):
                copy(k).wait_send()
                return 0

            lax.fori_loop(*span, passed, 0)

    o_gate[...] = acc[0].astype(bf16)
    o_up[...] = acc[1].astype(bf16)
    o_down[...] = acc_down[...].astype(bf16)


def write_out(*refs):
    sources, targets, sems = refs[:3], refs[3:6], refs[6]
    copies = [pltpu.make_async_copy(source, target, sems.at[i]) for i, (source, target) in enumerate(zip(sources, targets))]
    for copy in copies:
        copy.start()
    for copy in copies:
        copy.wait()


def solution(mesh):
    stages = mesh.shape["pp"]

    def step(x, dy, w_gate, w_up, w_down):
        micro, tokens, d = x.shape
        ff = w_gate.shape[2]
        per = tokens // ROWS
        chunks = micro * per
        x, dy = (v.reshape(chunks, ROWS, d) for v in (x, dy))
        vmem, anywhere = pl.BlockSpec(memory_space=pltpu.VMEM), pl.BlockSpec(memory_space=pl.ANY)
        by_gate, by_up, by_down = pl.pallas_call(
            functools.partial(kernel, stages, chunks, per),
            out_shape=[pltpu.VMEM((d, ff), bf16)] * 2 + [pltpu.VMEM((ff, d), bf16)],
            in_specs=[anywhere] * 2 + [vmem] * 3,
            out_specs=[vmem] * 3,
            scratch_shapes=[
                pltpu.VMEM((chunks, ROWS, d), bf16),
                pltpu.VMEM((chunks, ROWS, d), bf16),
                pltpu.VMEM((RING, ROWS, d), bf16),
                pltpu.VMEM((RING, ROWS, d), bf16),
                pltpu.VMEM((ROWS, ff), bf16),
                pltpu.VMEM((tokens, d), bf16),
                pltpu.VMEM((tokens, ff), bf16),
                pltpu.VMEM((2, d, ff), f32),
                pltpu.VMEM((ff, d), f32),
                pltpu.VMEM((max(b - a for a, b in (F_SPLIT, B_SPLIT)), max(F_FAR, B_FAR), d), bf16),
                pltpu.VMEM((SLOTS, 2, ROWS, ff), f32),
                pltpu.SemaphoreType.DMA((chunks,)),
                pltpu.SemaphoreType.DMA((chunks,)),
                pltpu.SemaphoreType.DMA((RING,)),
                pltpu.SemaphoreType.DMA((RING,)),
                pltpu.SemaphoreType.DMA((chunks,)),
                pltpu.SemaphoreType.DMA((chunks,)),
                pltpu.SemaphoreType.DMA((chunks,)),
                pltpu.SemaphoreType.DMA((chunks,)),
                pltpu.SemaphoreType.DMA((RING,)),
            ],
            compiler_params=pltpu.CompilerParams(collective_id=0, has_side_effects=True, vmem_limit_bytes=VMEM_BYTES),
            cost_estimate=pl.CostEstimate(flops=22 * micro * tokens * d * ff, bytes_accessed=16 * d * ff, transcendentals=0),
        )(x, dy, w_gate[0], w_up[0], w_down[0])
        outs = pl.pallas_call(
            write_out,
            out_shape=[jax.ShapeDtypeStruct(v.shape, bf16) for v in (by_gate, by_up, by_down)],
            in_specs=[vmem] * 3,
            out_specs=[anywhere] * 3,
            scratch_shapes=[pltpu.SemaphoreType.DMA((3,))],
            compiler_params=pltpu.CompilerParams(vmem_limit_bytes=2**20),
        )(by_gate, by_up, by_down)
        return tuple(v[None] for v in outs)

    return jax.shard_map(
        step,
        mesh=mesh,
        in_specs=(P("rep", None, None),) * 2 + (P("pp", None, None),) * 3,
        out_specs=(P(("rep", "pp"), None, None),) * 3,
        check_vma=False,
    )
```

```python
import functools

import jax
import jax.numpy as jnp
from jax import lax
from jax.experimental import pallas as pl
from jax.experimental.pallas import tpu as pltpu
from jax.sharding import PartitionSpec as P

f32, bf16 = jnp.float32, jnp.bfloat16
MESH = pl.DeviceIdType.MESH
ROWS = 256
BLOCK = 256
RING = 4
LEAD = (28, 24, 15, 13, 8, 6, 2, 0)
CROSS = 3
F_RELAY, B_RELAY = 0, 7
F_FAR, B_FAR = 144, 112
F_SPLIT, B_SPLIT = (7, 31), (0, 20)
F_BEHIND, B_BEHIND = 10, 6
COVERED = ()
STASHED, SLOTS = (1, 2, 3, 4, 5, 6), 9
AWAY, OUTGOING, INCOMING, SOON = (1, 2, 3), 4, 4, 3
VMEM_BYTES = 60 * 2**20


def mm(a, b):
    return jnp.dot(a, b, preferred_element_type=f32)


def mm_nt(a, b):
    return lax.dot_general(a, b, (((1,), (1,)), ((), ())), preferred_element_type=f32)


def mm_tn(a, b):
    return lax.dot_general(a, b, (((0,), (0,)), ((), ())), preferred_element_type=f32)


def norm_of(h):
    wide = h.astype(f32)
    return wide, lax.rsqrt(jnp.mean(wide * wide, -1, keepdims=True) + 1e-6)


def blocks(ff):
    return [slice(at, at + BLOCK) for at in range(0, ff, BLOCK)]


def forward(h, wg, wu, wd, hidden, stash=None):
    wide, scale = norm_of(h)
    a = (wide * scale).astype(bf16)
    for c in blocks(hidden.shape[1]):
        gate, up = mm(a, wg[:, c]), mm(a, wu[:, c])
        if stash is not None:
            stash[0, :, c], stash[1, :, c] = gate, up
        hidden[:, c] = (gate * jax.nn.sigmoid(gate) * up).astype(bf16)
    return h + mm(hidden[...], wd[...]).astype(bf16)


def backward(h, by_y, wg, wu, wd, a_all, hid_all, by_gate, by_up, rows, stash=None):
    wide, scale = norm_of(h)
    a = (wide * scale).astype(bf16)
    a_all[rows, :] = a
    for c in blocks(hid_all.shape[1]):
        gate, up = (mm(a, wg[:, c]), mm(a, wu[:, c])) if stash is None else (stash[0, :, c], stash[1, :, c])
        by_hid = mm_nt(by_y, wd[c, :]).astype(bf16).astype(f32)
        sig = jax.nn.sigmoid(gate)
        silu = gate * sig
        hid_all[rows, c] = (silu * up).astype(bf16)
        by_up[rows, c] = (by_hid * silu).astype(bf16)
        by_gate[rows, c] = ((by_hid * up) * (sig + silu * (1.0 - sig))).astype(bf16)
    return wide, scale


def backward_input(wide, scale, by_y, wg, wu, by_gate, by_up, rows):
    by_a = mm_nt(by_gate[rows, :], wg[...]).astype(bf16) + mm_nt(by_up[rows, :], wu[...]).astype(bf16)
    by_a = by_a.astype(f32)
    inner = jnp.sum(by_a * wide, -1, keepdims=True) * (1.0 / wide.shape[1])
    return by_y + (by_a * scale - wide * (scale * scale * scale * inner)).astype(bf16)


def kernel(stages, chunks, per, x, dy, wg, wu, wd, o_gate, o_up, o_down, store, kept, came, f_out, b_out, hidden, a_all, hid_all,
           acc, acc_down, relay, stash, f_in, b_in, f_sent, b_sent, f_round, b_round, r_in, r_sent, x_sent, s_out, s_back):
    me = lax.axis_index("pp")
    first, last = me == 0, me == stages - 1
    lead = sum(jnp.where(me == i, n, 0) for i, n in enumerate(LEAD))
    ff = hidden.shape[1]
    by_gate, by_up = o_gate, o_up

    barrier = pltpu.get_barrier_semaphore()

    @pl.when(jnp.logical_not(last))
    def _():
        pl.semaphore_signal(barrier, inc=1, device_id={"pp": me + 1}, device_id_type=MESH)

    @pl.when(jnp.logical_not(first))
    def _():
        pl.semaphore_signal(barrier, inc=1, device_id={"pp": me - 1}, device_id_type=MESH)

    pairs = [(CROSS, F_RELAY), (F_RELAY, CROSS + 1), (CROSS + 1, B_RELAY), (B_RELAY, CROSS)]
    for one, other in pairs + [(b, a) for a, b in pairs]:

        @pl.when(me == one)
        def _():
            pl.semaphore_signal(barrier, inc=1, device_id={"pp": other}, device_id_type=MESH)

    greeted = jnp.where(first | last, 1, 2) + sum(jnp.where(me == one, 1, 0) for pair in pairs for one in pair)
    pl.semaphore_wait(barrier, greeted)

    def load(source, target, sems):
        def one(k, _):
            pltpu.make_async_copy(source.at[k], target.at[k], sems.at[k]).start()
            return 0

        lax.fori_loop(0, chunks, one, 0)

    @pl.when(first)
    def _():
        load(x, kept, f_in)

    @pl.when(last)
    def _():
        load(dy, came, b_in)

    acc[...] = jnp.zeros_like(acc)
    acc_down[...] = jnp.zeros_like(acc_down)

    def send(k, out, into, sent, arrived, to):
        slot = lax.rem(k, RING)
        return pltpu.make_async_remote_copy(
            src_ref=out.at[slot], dst_ref=into.at[k], send_sem=sent.at[slot], recv_sem=arrived.at[k], device_id={"pp": to}, device_id_type=MESH
        )

    def f_split(k):
        return (k >= F_SPLIT[0]) & (k < F_SPLIT[1])

    def b_split(k):
        return (k >= B_SPLIT[0]) & (k < B_SPLIT[1])

    f_cut, b_cut = ((pl.ds(0, ROWS - far), pl.ds(ROWS - far, far), pl.ds(0, far), span[0]) for far, span in ((F_FAR, F_SPLIT), (B_FAR, B_SPLIT)))

    def halves(k, out, into, sent, arrived, to, by, cut):
        slot = lax.rem(k, RING)
        near, far, at, base = cut
        return (
            pltpu.make_async_remote_copy(
                src_ref=out.at[slot, near], dst_ref=into.at[k, near], send_sem=sent.at[slot], recv_sem=arrived.at[k], device_id={"pp": to},
                device_id_type=MESH,
            ),
            pltpu.make_async_remote_copy(
                src_ref=out.at[slot, far], dst_ref=relay.at[k - base, at], send_sem=x_sent.at[slot], recv_sem=r_in.at[k], device_id={"pp": by},
                device_id_type=MESH,
            ),
        )

    def pass_on(k, into, round_, to, cut):
        return pltpu.make_async_remote_copy(
            src_ref=relay.at[k - cut[3], cut[2]], dst_ref=into.at[k, cut[1]], send_sem=r_sent.at[k], recv_sem=round_.at[k], device_id={"pp": to},
            device_id_type=MESH,
        )

    f_pass = lambda k: pass_on(k, kept, f_round, CROSS + 1, f_cut)
    b_pass = lambda k: pass_on(k, came, b_round, CROSS, b_cut)

    def either(split, whole, parts):
        @pl.when(jnp.logical_not(split))
        def _():
            whole()

        @pl.when(split)
        def _():
            parts()

    def f_do(k, what):
        def parts():
            for copy in halves(k, f_out, kept, f_sent, f_in, CROSS + 1, F_RELAY, f_cut):
                what(copy)

        either((me == CROSS) & f_split(k), lambda: what(send(k, f_out, kept, f_sent, f_in, me + 1)), parts)

    def b_do(k, what):
        def parts():
            for copy in halves(k, b_out, came, b_sent, b_in, CROSS, B_RELAY, b_cut):
                what(copy)

        either((me == CROSS + 1) & b_split(k), lambda: what(send(k, b_out, came, b_sent, b_in, me - 1)), parts)

    start, wait_send = lambda copy: copy.start(), lambda copy: copy.wait_send()

    def arrived(k, into, sems, round_, split, cut):
        def parts():
            for rows, sem in zip(cut, (sems, round_)):
                pltpu.make_async_copy(into.at[k, rows], into.at[k, rows], sem.at[k]).wait()

        either(split, lambda: pltpu.make_async_copy(into.at[k], into.at[k], sems.at[k]).wait(), parts)

    stashes = sum(jnp.where(me == i, 1, 0) for i in STASHED) > 0

    away = sum([jnp.where(me == i, 1, 0) for i in AWAY], 0) > 0
    covers = sum([jnp.where(me == i, 1, 0) for i in COVERED], 0) > 0
    middle = jnp.logical_not(first | stashes)

    def take(t, _):
        for by, behind, split, copy, cut in ((F_RELAY, F_BEHIND, f_split, f_pass, f_cut), (B_RELAY, B_BEHIND, b_split, b_pass, b_cut)):

            @pl.when((me == by) & (t >= behind) & split(t - behind))
            def _():
                here = relay.at[t - behind - cut[3], cut[2]]
                pltpu.make_async_copy(here, here, r_in.at[t - behind]).wait()
                copy(t - behind).start()

        k, j = t, t - lead
        has_f, has_b = (k < chunks) & jnp.logical_not(last), (j >= 0) & (j < chunks)
        rows = pl.ds(pl.multiple_of(lax.rem(j + chunks, per) * ROWS, ROWS), ROWS)
        out = jnp.logical_not(first)

        def weights():
            by_out = jnp.concatenate([came[j - per + i] for i in range(per)], axis=0)
            for c in blocks(ff):
                acc[0, :, c] += mm_tn(a_all[...], by_gate[:, c]).astype(bf16).astype(f32)
                acc[1, :, c] += mm_tn(a_all[...], by_up[:, c]).astype(bf16).astype(f32)
                acc_down[c, :] += mm_tn(hid_all[:, c], by_out).astype(bf16).astype(f32)

        due = (j >= per) & (j <= chunks) & (lax.rem(j + chunks, per) == 0)
        f_slot = jnp.where(away, lax.rem(k, OUTGOING), lax.rem(k, SLOTS))
        b_slot = jnp.where(away, OUTGOING + lax.rem(j + chunks, INCOMING), lax.rem(j + SLOTS * chunks, SLOTS))

        def put(k):
            slot = lax.rem(k, OUTGOING)
            return pltpu.make_async_copy(stash.at[slot], store.at[k], s_out.at[slot])

        def get(j):
            slot = lax.rem(j, INCOMING)
            return pltpu.make_async_copy(store.at[j], stash.at[OUTGOING + slot], s_back.at[slot])

        @pl.when(away & (k >= OUTGOING) & (k < chunks + OUTGOING))
        def _():
            put(k - OUTGOING).wait()

        @pl.when(away & (j + SOON >= 0) & (j + SOON < chunks))
        def _():
            get(j + SOON).start()

        covered = due & has_f & covers
        pl.when(due & jnp.logical_not(covered))(weights)

        @pl.when(k < chunks)
        def _():
            arrived(k, kept, f_in, f_round, (me == CROSS + 1) & f_split(k), f_cut)

        @pl.when(has_f & (k >= RING))
        def _():
            f_do(k - RING, wait_send)

        def await_b():
            arrived(j, came, b_in, b_round, (me == CROSS) & b_split(j), b_cut)

            @pl.when(out & (j >= RING))
            def _():
                b_do(j - RING, wait_send)

            @pl.when(away)
            def _():
                get(j).wait()

        def work(forth, back, whole=True, stashed=False):
            if back:
                kept_of = stash.at[b_slot] if stashed else None
                wide, scale = backward(kept[j], came[j], wg, wu, wd, a_all, hid_all, by_gate, by_up, rows, kept_of)
                if whole:
                    b_out[lax.rem(j, RING)] = backward_input(wide, scale, came[j], wg, wu, by_gate, by_up, rows)
            if forth:
                f_out[lax.rem(k, RING)] = forward(kept[k], wg, wu, wd, hidden, stash.at[f_slot] if stashed else None)

        @pl.when(covered)
        def _():
            weights()
            work(True, False, stashed=True)

        pl.when(has_f & jnp.logical_not(covered))(lambda: work(True, False, stashed=True))

        @pl.when(has_f)
        def _():
            f_do(k, start)

        @pl.when(has_f & away)
        def _():
            put(k).start()

        pl.when(has_b)(await_b)
        pl.when(has_b & first)(lambda: work(False, True, whole=False))
        pl.when(has_b & middle)(lambda: work(False, True))
        pl.when(has_b & stashes)(lambda: work(False, True, stashed=True))

        @pl.when(has_b & out)
        def _():
            b_do(j, start)

        return 0

    steps = chunks + jnp.maximum(lead + 1, jnp.where(me == F_RELAY, F_BEHIND, jnp.where(me == B_RELAY, B_BEHIND, 0)))
    lax.fori_loop(0, steps, take, 0)

    def drain(i, _):
        @pl.when(jnp.logical_not(last))
        def _():
            f_do(chunks - RING + i, wait_send)

        @pl.when(jnp.logical_not(first))
        def _():
            b_do(chunks - RING + i, wait_send)

        return 0

    lax.fori_loop(0, RING, drain, 0)
    for by, span, copy in ((F_RELAY, F_SPLIT, f_pass), (B_RELAY, B_SPLIT, b_pass)):

        @pl.when(me == by)
        def _():
            def passed(k, _):
                copy(k).wait_send()
                return 0

            lax.fori_loop(*span, passed, 0)

    o_gate[...] = acc[0].astype(bf16)
    o_up[...] = acc[1].astype(bf16)
    o_down[...] = acc_down[...].astype(bf16)


def write_out(*refs):
    sources, targets, sems = refs[:3], refs[3:6], refs[6]
    copies = [pltpu.make_async_copy(source, target, sems.at[i]) for i, (source, target) in enumerate(zip(sources, targets))]
    for copy in copies:
        copy.start()
    for copy in copies:
        copy.wait()


def solution(mesh):
    stages = mesh.shape["pp"]

    def step(x, dy, w_gate, w_up, w_down):
        micro, tokens, d = x.shape
        ff = w_gate.shape[2]
        per = tokens // ROWS
        chunks = micro * per
        x, dy = (v.reshape(chunks, ROWS, d) for v in (x, dy))
        vmem, anywhere = pl.BlockSpec(memory_space=pltpu.VMEM), pl.BlockSpec(memory_space=pl.ANY)
        by_gate, by_up, by_down, _ = pl.pallas_call(
            functools.partial(kernel, stages, chunks, per),
            out_shape=[pltpu.VMEM((d, ff), bf16)] * 2 + [pltpu.VMEM((ff, d), bf16), jax.ShapeDtypeStruct((chunks, 2, ROWS, ff), f32)],
            in_specs=[anywhere] * 2 + [vmem] * 3,
            out_specs=[vmem] * 3 + [anywhere],
            scratch_shapes=[
                pltpu.VMEM((chunks, ROWS, d), bf16),
                pltpu.VMEM((chunks, ROWS, d), bf16),
                pltpu.VMEM((RING, ROWS, d), bf16),
                pltpu.VMEM((RING, ROWS, d), bf16),
                pltpu.VMEM((ROWS, ff), bf16),
                pltpu.VMEM((tokens, d), bf16),
                pltpu.VMEM((tokens, ff), bf16),
                pltpu.VMEM((2, d, ff), f32),
                pltpu.VMEM((ff, d), f32),
                pltpu.VMEM((max(b - a for a, b in (F_SPLIT, B_SPLIT)), max(F_FAR, B_FAR), d), bf16),
                pltpu.VMEM((SLOTS, 2, ROWS, ff), f32),
                pltpu.SemaphoreType.DMA((chunks,)),
                pltpu.SemaphoreType.DMA((chunks,)),
                pltpu.SemaphoreType.DMA((RING,)),
                pltpu.SemaphoreType.DMA((RING,)),
                pltpu.SemaphoreType.DMA((chunks,)),
                pltpu.SemaphoreType.DMA((chunks,)),
                pltpu.SemaphoreType.DMA((chunks,)),
                pltpu.SemaphoreType.DMA((chunks,)),
                pltpu.SemaphoreType.DMA((RING,)),
                pltpu.SemaphoreType.DMA((OUTGOING,)),
                pltpu.SemaphoreType.DMA((INCOMING,)),
            ],
            compiler_params=pltpu.CompilerParams(collective_id=0, has_side_effects=True, vmem_limit_bytes=VMEM_BYTES),
            cost_estimate=pl.CostEstimate(flops=22 * micro * tokens * d * ff, bytes_accessed=16 * d * ff, transcendentals=0),
        )(x, dy, w_gate[0], w_up[0], w_down[0])
        outs = pl.pallas_call(
            write_out,
            out_shape=[jax.ShapeDtypeStruct(v.shape, bf16) for v in (by_gate, by_up, by_down)],
            in_specs=[vmem] * 3,
            out_specs=[anywhere] * 3,
            scratch_shapes=[pltpu.SemaphoreType.DMA((3,))],
            compiler_params=pltpu.CompilerParams(vmem_limit_bytes=2**20),
        )(by_gate, by_up, by_down)
        return tuple(v[None] for v in outs)

    return jax.shard_map(
        step,
        mesh=mesh,
        in_specs=(P("rep", None, None),) * 2 + (P("pp", None, None),) * 3,
        out_specs=(P(("rep", "pp"), None, None),) * 3,
        check_vma=False,
    )
```

```python
import functools

import jax
import jax.numpy as jnp
from jax import lax
from jax.experimental import pallas as pl
from jax.experimental.pallas import tpu as pltpu
from jax.sharding import PartitionSpec as P

f32, bf16 = jnp.float32, jnp.bfloat16
MESH = pl.DeviceIdType.MESH
ROWS = 256
BLOCK = 256
RING = 4
LEAD = (28, 24, 15, 13, 8, 6, 2, 0)
CROSS = 3
F_RELAY, B_RELAY = 0, 7
F_FAR, B_FAR = 144, 112
F_SPLIT, B_SPLIT = (7, 31), (0, 20)
F_BEHIND, B_BEHIND = 10, 6
COVERED = ()
STASHED, SLOTS = (1, 2, 3, 4, 5, 6), 7
AWAY, OUTGOING, INCOMING, SOON = (1, 2, 3, 4), 3, 4, 3
VMEM_BYTES = 60 * 2**20


def mm(a, b):
    return jnp.dot(a, b, preferred_element_type=f32)


def mm_nt(a, b):
    return lax.dot_general(a, b, (((1,), (1,)), ((), ())), preferred_element_type=f32)


def mm_tn(a, b):
    return lax.dot_general(a, b, (((0,), (0,)), ((), ())), preferred_element_type=f32)


def norm_of(h):
    wide = h.astype(f32)
    return wide, lax.rsqrt(jnp.mean(wide * wide, -1, keepdims=True) + 1e-6)


def blocks(ff):
    return [slice(at, at + BLOCK) for at in range(0, ff, BLOCK)]


def forward(h, wg, wu, wd, stash, hidden):
    wide, scale = norm_of(h)
    a = (wide * scale).astype(bf16)
    for c in blocks(hidden.shape[1]):
        gate, up = mm(a, wg[:, c]), mm(a, wu[:, c])
        sig = jax.nn.sigmoid(gate)
        silu = gate * sig
        stash[0, :, c], stash[1, :, c] = silu, up * (sig + silu * (1.0 - sig))
        hidden[:, c] = (silu * up).astype(bf16)
    return h + mm(hidden[...], wd[...]).astype(bf16)


def backward(h, by_y, wg, wu, wd, a_all, hid_all, by_gate, by_up, rows, stash=None, hidden=None):
    wide, scale = norm_of(h)
    a = (wide * scale).astype(bf16)
    a_all[rows, :] = a
    for c in blocks(hid_all.shape[1]):
        if stash is None:
            gate, up = mm(a, wg[:, c]), mm(a, wu[:, c])
            sig = jax.nn.sigmoid(gate)
            silu = gate * sig
            slope = up * (sig + silu * (1.0 - sig))
            hid_all[rows, c] = (silu * up).astype(bf16)
        else:
            silu, slope = stash[0, :, c], stash[1, :, c]
            hid_all[rows, c] = hidden[:, c]
        by_hid = mm_nt(by_y, wd[c, :]).astype(bf16).astype(f32)
        by_up[rows, c] = (by_hid * silu).astype(bf16)
        by_gate[rows, c] = (by_hid * slope).astype(bf16)
    return wide, scale


def backward_input(wide, scale, by_y, wg, wu, by_gate, by_up, rows):
    by_a = mm_nt(by_gate[rows, :], wg[...]).astype(bf16) + mm_nt(by_up[rows, :], wu[...]).astype(bf16)
    by_a = by_a.astype(f32)
    inner = jnp.sum(by_a * wide, -1, keepdims=True) * (1.0 / wide.shape[1])
    return by_y + (by_a * scale - wide * (scale * scale * scale * inner)).astype(bf16)


def kernel(stages, chunks, per, x, dy, wg, wu, wd, o_gate, o_up, o_down, store, store_hid, kept, came, f_out, b_out, hidden, a_all, hid_all,
           acc, acc_down, relay, stash, f_in, b_in, f_sent, b_sent, f_round, b_round, r_in, r_sent, x_sent, s_out, s_back, h_out, h_back):
    me = lax.axis_index("pp")
    first, last = me == 0, me == stages - 1
    lead = sum(jnp.where(me == i, n, 0) for i, n in enumerate(LEAD))
    ff = hid_all.shape[1]
    by_gate, by_up = o_gate, o_up

    barrier = pltpu.get_barrier_semaphore()

    @pl.when(jnp.logical_not(last))
    def _():
        pl.semaphore_signal(barrier, inc=1, device_id={"pp": me + 1}, device_id_type=MESH)

    @pl.when(jnp.logical_not(first))
    def _():
        pl.semaphore_signal(barrier, inc=1, device_id={"pp": me - 1}, device_id_type=MESH)

    pairs = [(CROSS, F_RELAY), (F_RELAY, CROSS + 1), (CROSS + 1, B_RELAY), (B_RELAY, CROSS)]
    for one, other in pairs + [(b, a) for a, b in pairs]:

        @pl.when(me == one)
        def _():
            pl.semaphore_signal(barrier, inc=1, device_id={"pp": other}, device_id_type=MESH)

    greeted = jnp.where(first | last, 1, 2) + sum(jnp.where(me == one, 1, 0) for pair in pairs for one in pair)
    pl.semaphore_wait(barrier, greeted)

    def load(source, target, sems):
        def one(k, _):
            pltpu.make_async_copy(source.at[k], target.at[k], sems.at[k]).start()
            return 0

        lax.fori_loop(0, chunks, one, 0)

    @pl.when(first)
    def _():
        load(x, kept, f_in)

    @pl.when(last)
    def _():
        load(dy, came, b_in)

    acc[...] = jnp.zeros_like(acc)
    acc_down[...] = jnp.zeros_like(acc_down)

    def send(k, out, into, sent, arrived, to):
        slot = lax.rem(k, RING)
        return pltpu.make_async_remote_copy(
            src_ref=out.at[slot], dst_ref=into.at[k], send_sem=sent.at[slot], recv_sem=arrived.at[k], device_id={"pp": to}, device_id_type=MESH
        )

    def f_split(k):
        return (k >= F_SPLIT[0]) & (k < F_SPLIT[1])

    def b_split(k):
        return (k >= B_SPLIT[0]) & (k < B_SPLIT[1])

    f_cut, b_cut = ((pl.ds(0, ROWS - far), pl.ds(ROWS - far, far), pl.ds(0, far), span[0]) for far, span in ((F_FAR, F_SPLIT), (B_FAR, B_SPLIT)))

    def halves(k, out, into, sent, arrived, to, by, cut):
        slot = lax.rem(k, RING)
        near, far, at, base = cut
        return (
            pltpu.make_async_remote_copy(
                src_ref=out.at[slot, near], dst_ref=into.at[k, near], send_sem=sent.at[slot], recv_sem=arrived.at[k], device_id={"pp": to},
                device_id_type=MESH,
            ),
            pltpu.make_async_remote_copy(
                src_ref=out.at[slot, far], dst_ref=relay.at[k - base, at], send_sem=x_sent.at[slot], recv_sem=r_in.at[k], device_id={"pp": by},
                device_id_type=MESH,
            ),
        )

    def pass_on(k, into, round_, to, cut):
        return pltpu.make_async_remote_copy(
            src_ref=relay.at[k - cut[3], cut[2]], dst_ref=into.at[k, cut[1]], send_sem=r_sent.at[k], recv_sem=round_.at[k], device_id={"pp": to},
            device_id_type=MESH,
        )

    f_pass = lambda k: pass_on(k, kept, f_round, CROSS + 1, f_cut)
    b_pass = lambda k: pass_on(k, came, b_round, CROSS, b_cut)

    def either(split, whole, parts):
        @pl.when(jnp.logical_not(split))
        def _():
            whole()

        @pl.when(split)
        def _():
            parts()

    def f_do(k, what):
        def parts():
            for copy in halves(k, f_out, kept, f_sent, f_in, CROSS + 1, F_RELAY, f_cut):
                what(copy)

        either((me == CROSS) & f_split(k), lambda: what(send(k, f_out, kept, f_sent, f_in, me + 1)), parts)

    def b_do(k, what):
        def parts():
            for copy in halves(k, b_out, came, b_sent, b_in, CROSS, B_RELAY, b_cut):
                what(copy)

        either((me == CROSS + 1) & b_split(k), lambda: what(send(k, b_out, came, b_sent, b_in, me - 1)), parts)

    start, wait_send = lambda copy: copy.start(), lambda copy: copy.wait_send()

    def arrived(k, into, sems, round_, split, cut):
        def parts():
            for rows, sem in zip(cut, (sems, round_)):
                pltpu.make_async_copy(into.at[k, rows], into.at[k, rows], sem.at[k]).wait()

        either(split, lambda: pltpu.make_async_copy(into.at[k], into.at[k], sems.at[k]).wait(), parts)

    stashes = sum(jnp.where(me == i, 1, 0) for i in STASHED) > 0

    away = sum([jnp.where(me == i, 1, 0) for i in AWAY], 0) > 0
    covers = sum([jnp.where(me == i, 1, 0) for i in COVERED], 0) > 0
    middle = jnp.logical_not(first | stashes)

    def take(t, _):
        for by, behind, split, copy, cut in ((F_RELAY, F_BEHIND, f_split, f_pass, f_cut), (B_RELAY, B_BEHIND, b_split, b_pass, b_cut)):

            @pl.when((me == by) & (t >= behind) & split(t - behind))
            def _():
                here = relay.at[t - behind - cut[3], cut[2]]
                pltpu.make_async_copy(here, here, r_in.at[t - behind]).wait()
                copy(t - behind).start()

        k, j = t, t - lead
        has_f, has_b = (k < chunks) & jnp.logical_not(last), (j >= 0) & (j < chunks)
        rows = pl.ds(pl.multiple_of(lax.rem(j + chunks, per) * ROWS, ROWS), ROWS)
        out = jnp.logical_not(first)

        def weights():
            by_out = jnp.concatenate([came[j - per + i] for i in range(per)], axis=0)
            for c in blocks(ff):
                acc[0, :, c] += mm_tn(a_all[...], by_gate[:, c]).astype(bf16).astype(f32)
                acc[1, :, c] += mm_tn(a_all[...], by_up[:, c]).astype(bf16).astype(f32)
                acc_down[c, :] += mm_tn(hid_all[:, c], by_out).astype(bf16).astype(f32)

        due = (j >= per) & (j <= chunks) & (lax.rem(j + chunks, per) == 0)
        f_slot = jnp.where(away, lax.rem(k, OUTGOING), lax.rem(k, SLOTS))
        b_slot = jnp.where(away, OUTGOING + lax.rem(j + chunks, INCOMING), lax.rem(j + SLOTS * chunks, SLOTS))

        def put(k):
            slot = lax.rem(k, OUTGOING)
            return (
                pltpu.make_async_copy(stash.at[slot], store.at[k], s_out.at[slot]),
                pltpu.make_async_copy(hidden.at[slot], store_hid.at[k], h_out.at[slot]),
            )

        def get(j):
            slot = lax.rem(j, INCOMING)
            return (
                pltpu.make_async_copy(store.at[j], stash.at[OUTGOING + slot], s_back.at[slot]),
                pltpu.make_async_copy(store_hid.at[j], hidden.at[OUTGOING + slot], h_back.at[slot]),
            )

        @pl.when(away & (k >= OUTGOING) & (k < chunks + OUTGOING))
        def _():
            for copy in put(k - OUTGOING):
                copy.wait()

        @pl.when(away & (j + SOON >= 0) & (j + SOON < chunks))
        def _():
            for copy in get(j + SOON):
                copy.start()

        covered = due & has_f & covers
        pl.when(due & jnp.logical_not(covered))(weights)

        @pl.when(k < chunks)
        def _():
            arrived(k, kept, f_in, f_round, (me == CROSS + 1) & f_split(k), f_cut)

        @pl.when(has_f & (k >= RING))
        def _():
            f_do(k - RING, wait_send)

        def await_b():
            arrived(j, came, b_in, b_round, (me == CROSS) & b_split(j), b_cut)

            @pl.when(out & (j >= RING))
            def _():
                b_do(j - RING, wait_send)

            @pl.when(away)
            def _():
                for copy in get(j):
                    copy.wait()

        def work(forth, back, whole=True, stashed=False):
            if back:
                kept_of = (stash.at[b_slot], hidden.at[b_slot]) if stashed else ()
                wide, scale = backward(kept[j], came[j], wg, wu, wd, a_all, hid_all, by_gate, by_up, rows, *kept_of)
                if whole:
                    b_out[lax.rem(j, RING)] = backward_input(wide, scale, came[j], wg, wu, by_gate, by_up, rows)
            if forth:
                f_out[lax.rem(k, RING)] = forward(kept[k], wg, wu, wd, stash.at[f_slot], hidden.at[f_slot])

        @pl.when(covered)
        def _():
            weights()
            work(True, False, stashed=True)

        pl.when(has_f & jnp.logical_not(covered))(lambda: work(True, False, stashed=True))

        @pl.when(has_f)
        def _():
            f_do(k, start)

        @pl.when(has_f & away)
        def _():
            for copy in put(k):
                copy.start()

        pl.when(has_b)(await_b)
        pl.when(has_b & first)(lambda: work(False, True, whole=False))
        pl.when(has_b & middle)(lambda: work(False, True))
        pl.when(has_b & stashes)(lambda: work(False, True, stashed=True))

        @pl.when(has_b & out)
        def _():
            b_do(j, start)

        return 0

    steps = chunks + jnp.maximum(lead + 1, jnp.where(me == F_RELAY, F_BEHIND, jnp.where(me == B_RELAY, B_BEHIND, 0)))
    lax.fori_loop(0, steps, take, 0)

    def drain(i, _):
        @pl.when(jnp.logical_not(last))
        def _():
            f_do(chunks - RING + i, wait_send)

        @pl.when(jnp.logical_not(first))
        def _():
            b_do(chunks - RING + i, wait_send)

        return 0

    lax.fori_loop(0, RING, drain, 0)
    for by, span, copy in ((F_RELAY, F_SPLIT, f_pass), (B_RELAY, B_SPLIT, b_pass)):

        @pl.when(me == by)
        def _():
            def passed(k, _):
                copy(k).wait_send()
                return 0

            lax.fori_loop(*span, passed, 0)

    o_gate[...] = acc[0].astype(bf16)
    o_up[...] = acc[1].astype(bf16)
    o_down[...] = acc_down[...].astype(bf16)


def write_out(*refs):
    sources, targets, sems = refs[:3], refs[3:6], refs[6]
    copies = [pltpu.make_async_copy(source, target, sems.at[i]) for i, (source, target) in enumerate(zip(sources, targets))]
    for copy in copies:
        copy.start()
    for copy in copies:
        copy.wait()


def solution(mesh):
    stages = mesh.shape["pp"]

    def step(x, dy, w_gate, w_up, w_down):
        micro, tokens, d = x.shape
        ff = w_gate.shape[2]
        per = tokens // ROWS
        chunks = micro * per
        x, dy = (v.reshape(chunks, ROWS, d) for v in (x, dy))
        vmem, anywhere = pl.BlockSpec(memory_space=pltpu.VMEM), pl.BlockSpec(memory_space=pl.ANY)
        by_gate, by_up, by_down, *_ = pl.pallas_call(
            functools.partial(kernel, stages, chunks, per),
            out_shape=[pltpu.VMEM((d, ff), bf16)] * 2 + [pltpu.VMEM((ff, d), bf16), jax.ShapeDtypeStruct((chunks, 2, ROWS, ff), f32), jax.ShapeDtypeStruct((chunks, ROWS, ff), bf16)],
            in_specs=[anywhere] * 2 + [vmem] * 3,
            out_specs=[vmem] * 3 + [anywhere] * 2,
            scratch_shapes=[
                pltpu.VMEM((chunks, ROWS, d), bf16),
                pltpu.VMEM((chunks, ROWS, d), bf16),
                pltpu.VMEM((RING, ROWS, d), bf16),
                pltpu.VMEM((RING, ROWS, d), bf16),
                pltpu.VMEM((SLOTS, ROWS, ff), bf16),
                pltpu.VMEM((tokens, d), bf16),
                pltpu.VMEM((tokens, ff), bf16),
                pltpu.VMEM((2, d, ff), f32),
                pltpu.VMEM((ff, d), f32),
                pltpu.VMEM((max(b - a for a, b in (F_SPLIT, B_SPLIT)), max(F_FAR, B_FAR), d), bf16),
                pltpu.VMEM((SLOTS, 2, ROWS, ff), f32),
                pltpu.SemaphoreType.DMA((chunks,)),
                pltpu.SemaphoreType.DMA((chunks,)),
                pltpu.SemaphoreType.DMA((RING,)),
                pltpu.SemaphoreType.DMA((RING,)),
                pltpu.SemaphoreType.DMA((chunks,)),
                pltpu.SemaphoreType.DMA((chunks,)),
                pltpu.SemaphoreType.DMA((chunks,)),
                pltpu.SemaphoreType.DMA((chunks,)),
                pltpu.SemaphoreType.DMA((RING,)),
                pltpu.SemaphoreType.DMA((OUTGOING,)),
                pltpu.SemaphoreType.DMA((INCOMING,)),
                pltpu.SemaphoreType.DMA((OUTGOING,)),
                pltpu.SemaphoreType.DMA((INCOMING,)),
            ],
            compiler_params=pltpu.CompilerParams(collective_id=0, has_side_effects=True, vmem_limit_bytes=VMEM_BYTES),
            cost_estimate=pl.CostEstimate(flops=22 * micro * tokens * d * ff, bytes_accessed=16 * d * ff, transcendentals=0),
        )(x, dy, w_gate[0], w_up[0], w_down[0])
        outs = pl.pallas_call(
            write_out,
            out_shape=[jax.ShapeDtypeStruct(v.shape, bf16) for v in (by_gate, by_up, by_down)],
            in_specs=[vmem] * 3,
            out_specs=[anywhere] * 3,
            scratch_shapes=[pltpu.SemaphoreType.DMA((3,))],
            compiler_params=pltpu.CompilerParams(vmem_limit_bytes=2**20),
        )(by_gate, by_up, by_down)
        return tuple(v[None] for v in outs)

    return jax.shard_map(
        step,
        mesh=mesh,
        in_specs=(P("rep", None, None),) * 2 + (P("pp", None, None),) * 3,
        out_specs=(P(("rep", "pp"), None, None),) * 3,
        check_vma=False,
    )
```
